32 devices in a mesh: groups: 2 (over y), seq: 4 (over z), head: 2 (over x), dim: 2 (over core).
Axes of the slice: x: 2, y: 2, z: 4, core: 2. Of those that a mesh axis runs over, the one named last changes fastest.
Arguments:
- query: bfloat16 [4, 16, 1024, 128], P('groups', 'head', 'seq'), parts along dimension 0, may hold values from -6 to 6
- key: bfloat16 [4, 16, 1024, 128], P('groups', 'head', 'seq'), parts along dimension 0, may hold values from -6 to 6
- value: bfloat16 [4, 16, 128, 1024], P('groups', 'head', 'dim', 'seq'), parts along dimension 0, may hold values from -6 to 6
- out_gate: bfloat16 [4, 16, 128, 1024], P('groups', 'head', 'dim', 'seq'), parts along dimension 0, may hold values from -6 to 6
- beta: float32 [4, 16, 1024], P('groups', 'head', 'seq'), parts along dimension 0, may hold values from 0.1 to 0.9
- log_decay: float32 [4, 16, 1024], P('groups', 'head', 'seq'), parts along dimension 0, may hold values from -1 to 0, as said below
- lengths: int32 [4, 4], P('groups', 'seq'), parts along dimension 0, may hold values from 128 to 256
- norm_gain: float32 [128], P('dim'), may hold values from 0.1 to 1.9
Outputs:
- output: bfloat16 [4, 16, 128, 1024], P('groups', 'head', 'dim', 'seq'), parts along dimension 0
The draws below stay inside these ranges and needn't reach their ends.
There are 2 independent parts, one for each index of `groups`. The reference program is written for one: setup_inputs(seed, part) draws one part's arguments, and reference() takes and returns one part's arrays. A program takes and returns all parts, laid end to end along the dimension named above; an argument that names none is the same for every part. Nothing has to cross between parts.
Inputs may be any that keep to these rules, and one draw needn't show every extreme that they name: `log_decay`: negative.
All inputs are finite; a program needn't handle non-finite values.
Results may differ from the reference program's by a relative error of at most 0.001.
Values sent between devices are 32-bit elements; how exact they have to be, the bound alone decides.
A program may use at most 64 MiB of HBM per device.

```python
import math
import jax
import jax.numpy as jnp
from jax import lax

HEAD_COUNT = 16
DK = 128
DV = 128
TILE = 64
WINDOW = 4
TOK_DEV = 256
SEQUENCE_COUNT = 2
TOKEN_COUNT = 1024
N_SEQ = 4


def draw_log_decay(key, part):
    key_rows = jax.random.split(key, 7)
    chain_len = float(WINDOW * TOK_DEV)
    share = 0.5
    quick = jax.random.uniform(key_rows[0], (SEQUENCE_COUNT, HEAD_COUNT, 1)) < share
    fast_rate = jnp.exp(jax.random.uniform(key_rows[1], (SEQUENCE_COUNT, HEAD_COUNT, 1), minval=math.log(1.0 / 50.0), maxval=math.log(1.0 / 25.0)))
    slow_rate = jnp.exp(jax.random.uniform(key_rows[2], (SEQUENCE_COUNT, HEAD_COUNT, 1), minval=math.log(0.05 / chain_len), maxval=math.log(0.5 / chain_len)))
    baseline_rate = jnp.where(quick, fast_rate, slow_rate)
    block_multiplier = jax.random.uniform(key_rows[3], (SEQUENCE_COUNT, HEAD_COUNT, TOKEN_COUNT // TOK_DEV), minval=0.6, maxval=1.4)
    block_multiplier = jnp.repeat(block_multiplier, TOK_DEV, axis=-1)
    coarse_estimate = jax.random.uniform(key_rows[4], (SEQUENCE_COUNT, HEAD_COUNT, TOKEN_COUNT), minval=0.5, maxval=1.5)
    spike_struck = jax.random.uniform(key_rows[5], (SEQUENCE_COUNT, HEAD_COUNT, TOKEN_COUNT)) < 3.0 / TOKEN_COUNT
    spike_length = jax.random.uniform(key_rows[6], (SEQUENCE_COUNT, HEAD_COUNT, TOKEN_COUNT), minval=0.22, maxval=0.69)
    spike_event = jnp.where(spike_struck, spike_length, 0.0)
    return (-(baseline_rate * block_multiplier * coarse_estimate) - spike_event).astype(jnp.float32)


def draw_key(key, part):
    subkeys = jax.random.split(key, 3)
    sub_rank = max(DK // 8, 4)
    side_share = 0.0625
    side_scale = math.sqrt(side_share * DK / (DK - sub_rank - side_share * DK))
    basis_rows = jax.random.normal(subkeys[0], (SEQUENCE_COUNT, HEAD_COUNT, sub_rank, DK), dtype=jnp.float32)
    mixing = jax.random.normal(subkeys[1], (SEQUENCE_COUNT, HEAD_COUNT, TOKEN_COUNT, sub_rank), dtype=jnp.float32)
    spread_part = jax.random.normal(subkeys[2], (SEQUENCE_COUNT, HEAD_COUNT, TOKEN_COUNT, DK), dtype=jnp.float32)
    aligned = jnp.einsum('shtr,shrd->shtd', mixing, basis_rows) / math.sqrt(float(sub_rank))
    return jnp.clip(aligned + side_scale * spread_part, -6.0, 6.0).astype(jnp.bfloat16)


def with_ends(array, stream_key, least, largest):
    index_at = [jax.random.randint(jax.random.fold_in(stream_key, axis), (), 0, length) for axis, length in enumerate(array.shape)]
    main_axis = array.shape.index(max(array.shape))
    neighbour = index_at[:main_axis] + [(index_at[main_axis] + 1) % array.shape[main_axis]] + index_at[main_axis + 1:]
    return array.at[tuple(index_at)].set(least).at[tuple(neighbour)].set(largest)


def level_of(rng, shape, cuts, least, high):
    def one(dim, parts):
        heights = jax.random.uniform(jax.random.fold_in(jax.random.fold_in(rng, 6), dim), (parts,), jnp.float32, least / len(cuts), high / len(cuts))
        return jnp.repeat(jnp.exp(heights), shape[dim] // parts).reshape((-1,) + (1,) * (len(shape) - dim - 1))

    gain = one(*cuts[0])
    for cut in cuts[1:]:
        gain = gain * one(*cut)
    return gain


def normal_values(key, extent, deviation, most, cuts=(), kind=jnp.bfloat16):
    values = deviation * jax.random.normal(key, extent, jnp.float32)
    if cuts:
        values = values * level_of(key, extent, cuts, -0.22, 0.18)
    return jnp.clip(values, -most, most).astype(kind)


def setup_inputs(seed: int = 0, part: int = 0) -> dict:
    arg_keys = jax.random.split(jax.random.key(seed), 9)
    part_keys = jax.random.split(jax.random.fold_in(arg_keys[8], part), 9)
    query = normal_values(part_keys[0], (SEQUENCE_COUNT, HEAD_COUNT, TOKEN_COUNT, DK), 1.0, 6.0, ((1, 2), (2, 4)))
    key = draw_key(jax.random.fold_in(jax.random.fold_in(arg_keys[8], part), 71), part)
    value = normal_values(part_keys[2], (SEQUENCE_COUNT, HEAD_COUNT, DV, TOKEN_COUNT), 1.0, 6.0, ((1, 2), (2, 2), (3, 4)))
    out_gate = normal_values(part_keys[3], (SEQUENCE_COUNT, HEAD_COUNT, DV, TOKEN_COUNT), 1.0, 6.0, ((1, 2), (2, 2), (3, 4)))
    beta = jnp.clip(0.1 + 0.79999997 * jax.random.uniform(part_keys[4], (SEQUENCE_COUNT, HEAD_COUNT, TOKEN_COUNT), jnp.float32) ** level_of(part_keys[4], (SEQUENCE_COUNT, HEAD_COUNT, TOKEN_COUNT), ((1, 2), (2, 4)), -0.2, 0.2), 0.1, 0.9)
    log_decay = draw_log_decay(jax.random.fold_in(jax.random.fold_in(arg_keys[8], part), 71), part)
    lengths = with_ends(jax.random.randint(part_keys[6], (SEQUENCE_COUNT, N_SEQ), TOK_DEV // 2, TOK_DEV + 1), jax.random.fold_in(part_keys[6], 1), TOK_DEV // 2, TOK_DEV).astype(jnp.int32)
    norm_gain = jnp.clip(1.0 + 0.18 * jax.random.normal(arg_keys[7], (DV,), jnp.float32), 0.1, 1.9)
    return {"query": query, "key": key, "value": value, "out_gate": out_gate, "beta": beta, "log_decay": log_decay, "lengths": lengths, "norm_gain": norm_gain}


FULL_PREC = lax.Precision.HIGHEST

def apply_map(left, right):
    return jnp.matmul(left, right, precision=FULL_PREC)

def tile_terms(query_t, unit_t, value_t, eff_rate, eff_decay):
    tile_len = query_t.shape[-2]
    cumlog = jnp.cumsum(eff_decay, axis=-1)
    index_row = jnp.arange(tile_len)
    causal = index_row[:, None] >= index_row[None, :]
    before = index_row[:, None] > index_row[None, :]
    log_gap = cumlog[..., :, None] - cumlog[..., None, :]
    decays = jnp.where(causal, jnp.exp(jnp.where(causal, log_gap, 0.0)), 0.0)
    key_gram = jnp.einsum('...rd,...sd->...rs', unit_t, unit_t, precision=FULL_PREC)
    coupling = jnp.where(before, eff_rate[..., :, None] * decays * key_gram, 0.0)
    identity = jnp.eye(tile_len, dtype=coupling.dtype)
    right_side = jnp.concatenate([jnp.swapaxes(value_t, -1, -2) * eff_rate[..., None], unit_t * (eff_rate * jnp.exp(cumlog))[..., None]], axis=-1)
    solved = lax.linalg.triangular_solve(identity + coupling, right_side, left_side=True, lower=True, unit_diagonal=True)
    val_width = value_t.shape[-2]
    fresh_vals = solved[..., :val_width]
    key_mix = solved[..., val_width:]
    scores = decays * jnp.einsum('...rd,...sd->...rs', query_t, unit_t, precision=FULL_PREC)
    tile_end = cumlog[..., -1]
    carried = unit_t * jnp.exp(tile_end[..., None] - cumlog)[..., None]
    key_eye = jnp.eye(unit_t.shape[-1], dtype=carried.dtype)
    tile_map = jnp.exp(tile_end)[..., None, None] * key_eye - jnp.einsum('...rd,...re->...de', key_mix, carried, precision=FULL_PREC)
    tile_add = jnp.einsum('...rv,...rd->...vd', fresh_vals, carried, precision=FULL_PREC)
    return (fresh_vals, key_mix, scores, cumlog, tile_map, tile_add)

def tile_output(start_state, query_t, key_mix, fresh_vals, scores, cumlog):
    new_vals = fresh_vals - jnp.einsum('...rd,...vd->...rv', key_mix, start_state, precision=FULL_PREC)
    direct_term = jnp.einsum('...vd,...rd->...vr', start_state, query_t * jnp.exp(cumlog)[..., None], precision=FULL_PREC)
    return direct_term + jnp.einsum('...sv,...rs->...vr', new_vals, scores, precision=FULL_PREC)

def head_pass(head_items):
    query_h, unit_h, value_h, rate_h, decay_h = head_items
    tile_count = TOK_DEV // TILE
    query_t = query_h.astype(jnp.float32).reshape(SEQUENCE_COUNT, N_SEQ, tile_count, TILE, DK)
    unit_t = unit_h.reshape(SEQUENCE_COUNT, N_SEQ, tile_count, TILE, DK)
    value_t = value_h.astype(jnp.float32).reshape(SEQUENCE_COUNT, DV, N_SEQ, tile_count, TILE).transpose(0, 2, 3, 1, 4)
    rate_t = rate_h.reshape(SEQUENCE_COUNT, N_SEQ, tile_count, TILE)
    decay_t = decay_h.reshape(SEQUENCE_COUNT, N_SEQ, tile_count, TILE)
    fresh_vals, key_mix, scores, cumlog, tile_map, tile_add = tile_terms(query_t, unit_t, value_t, rate_t, decay_t)

    def advance(carried_pair, inputs):
        state_now, trans_now = carried_pair
        map_now, add_now = inputs
        return ((apply_map(state_now, map_now) + add_now, apply_map(trans_now, map_now)), None)
    initial = (jnp.zeros((SEQUENCE_COUNT, N_SEQ, DV, DK), jnp.float32), jnp.broadcast_to(jnp.eye(DK, dtype=jnp.float32), (SEQUENCE_COUNT, N_SEQ, DK, DK)))
    (block_end, block_map), _ = lax.scan(advance, initial, (jnp.moveaxis(tile_map, 2, 0), jnp.moveaxis(tile_add, 2, 0)))
    moving = block_end
    start_state = jnp.zeros_like(block_end)
    for hop_num in range(WINDOW):
        arrived = jnp.concatenate([jnp.zeros_like(moving[:, :1]), moving[:, :-1]], axis=1)
        start_state = start_state + arrived
        moving = apply_map(arrived, block_map)

    def emit_tile(state_now, inputs):
        query_x, mix_x, fresh_x, scores_x, cum_x, map_x, add_x = inputs
        result = tile_output(state_now, query_x, mix_x, fresh_x, scores_x, cum_x)
        return (apply_map(state_now, map_x) + add_x, result)
    _, tile_outs = lax.scan(emit_tile, start_state, tuple((jnp.moveaxis(item, 2, 0) for item in (query_t, key_mix, fresh_vals, scores, cumlog, tile_map, tile_add))))
    return tile_outs.transpose(1, 3, 2, 0, 4).reshape(SEQUENCE_COUNT, DV, TOKEN_COUNT)

def reference(query, key, value, out_gate, beta, log_decay, lengths, norm_gain):
    position = jnp.arange(TOKEN_COUNT)
    within = position % TOK_DEV
    owner_blk = (position // TOK_DEV).astype(jnp.int32)
    live_mask = (within[None, :] < lengths[:, owner_blk]).astype(jnp.float32)
    key_float = key.astype(jnp.float32)
    unit_key = key_float / jnp.sqrt(lax.optimization_barrier(jnp.sum(key_float * key_float, axis=-1, keepdims=True)) + 1e-06)
    eff_rate = beta * live_mask[:, None, :]
    eff_decay = log_decay * live_mask[:, None, :]
    raw_out = lax.map(head_pass, (jnp.swapaxes(query, 0, 1), jnp.swapaxes(unit_key, 0, 1), jnp.swapaxes(value, 0, 1), jnp.swapaxes(eff_rate, 0, 1), jnp.swapaxes(eff_decay, 0, 1)))
    raw_out = jnp.swapaxes(raw_out, 0, 1)
    mean_sq = lax.optimization_barrier(jnp.mean(raw_out * raw_out, axis=2))
    gated_out = raw_out * lax.rsqrt(mean_sq + 1e-06)[:, :, None, :] * norm_gain[None, None, :, None] * jax.nn.silu(out_gate.astype(jnp.float32)) * live_mask[:, None, None, :]
    return gated_out.astype(jnp.bfloat16)
```

```python
import functools

import jax
import jax.numpy as jnp
from jax import lax
from jax.experimental import pallas as pl
from jax.experimental.pallas import tpu as pltpu
from jax.sharding import PartitionSpec as P

WINDOW = 4
GROUP = 4
BASE = 16
TILE = 8
EPS = 1e-06
F32 = jnp.float32
BF16 = jnp.bfloat16


def dot(left, right):
    return jnp.dot(left, right, preferred_element_type=F32)


def dot_nt(left, right):
    return lax.dot_general(left, right, (((1,), (1,)), ((), ())), preferred_element_type=F32)


def split(x):
    high = x.astype(BF16)
    return high, (x - high.astype(F32)).astype(BF16)


def expand(x):
    half = x.shape[0]
    zero = jnp.zeros((half, half), x.dtype)
    return jnp.concatenate(
        [
            jnp.concatenate([x[:, :half], zero], axis=1),
            jnp.concatenate([zero, x[:, half:]], axis=1),
        ],
        axis=0,
    )


def corner_block(a, b, c):
    zero = jnp.zeros((c.shape[0], a.shape[1]), c.dtype)
    return jnp.concatenate(
        [jnp.concatenate([a, b], axis=1), jnp.concatenate([zero, c], axis=1)], axis=0
    )


def level_masks(half):
    row = lax.broadcasted_iota(jnp.int32, (half, 2 * half), 0)
    col = lax.broadcasted_iota(jnp.int32, (half, 2 * half), 1)
    col = jnp.where(col >= half, col - half, col)
    differ = jnp.bitwise_xor(row, col)
    masks = []
    size = BASE
    while size < half:
        masks.append((differ >= size) & (differ < 2 * size))
        size *= 2
    return [jnp.where(m, 1.0, 0.0).astype(BF16) for m in masks]


def tri_masks(half):
    row = lax.broadcasted_iota(jnp.int32, (half, half), 0)
    col = lax.broadcasted_iota(jnp.int32, (half, half), 1)
    return [jnp.where(m, 1.0, 0.0) for m in (row < col, row <= col, row == col)]


def block_ones(tokens):
    row = lax.broadcasted_iota(jnp.int32, (tokens, tokens), 0)
    col = lax.broadcasted_iota(jnp.int32, (tokens, tokens), 1)
    return jnp.where(jnp.bitwise_xor(row, col) < BASE, 1.0, 0.0).astype(BF16)


def lane_of(rows, tokens):
    return lax.broadcasted_iota(jnp.int32, (rows, tokens), 1)


def base_rows(packed):
    half, tokens = packed.shape
    lane = lane_of(BASE, tokens)
    block = jnp.bitwise_and(lane, half - 1) // BASE
    compact = jnp.zeros((BASE, tokens), F32)
    for b in range(half // BASE):
        compact = jnp.where(block == b, packed[b * BASE : (b + 1) * BASE], compact)
    inner = jnp.bitwise_and(lane, BASE - 1)
    pieces = []
    for j in range(1, BASE):
        rows = TILE if j <= TILE else BASE
        pieces.append(jnp.where(inner[:rows] == j, compact[:rows], 0.0))
    return jnp.concatenate(pieces, axis=0).astype(BF16)


def base_inverse(spread, half):
    tokens = spread.shape[1]
    offset, place = {}, 0
    for j in range(1, BASE):
        offset[j] = place
        place += TILE if j <= TILE else BASE
    lane = jnp.bitwise_and(lane_of(TILE, tokens), BASE - 1)
    row = lax.broadcasted_iota(jnp.int32, (TILE, tokens), 0)
    top = jnp.where(lane == row, 1.0, 0.0)
    low = jnp.where(lane == row + TILE, 1.0, 0.0)
    for j in range(BASE - 1, 0, -1):
        at = offset[j]
        if j > TILE:
            line = low[j - TILE : j - TILE + 1]
            low = low - spread[at + TILE : at + BASE] * line
        else:
            line = low[:1] if j == TILE else top[j : j + 1]
        top = top - spread[at : at + TILE] * line
    found = jnp.concatenate([top, low], axis=0)
    lane = lane_of(BASE, tokens)
    block = jnp.bitwise_and(lane, half - 1) // BASE
    return jnp.concatenate(
        [jnp.where(block == b, found, 0.0) for b in range(half // BASE)], axis=0
    ).astype(BF16)


def key_terms(items, masks, ones, tri):
    strict, _, eye = tri
    tokens = items[0][0].shape[0]
    half = tokens // 2
    stage = []
    for k, rate, cum in items:
        cum1, cum2 = cum[:, :half], cum[:, half:]
        col1 = jnp.sum(eye * cum1, axis=1, keepdims=True)
        col2 = jnp.sum(eye * cum2, axis=1, keepdims=True)
        d11 = jnp.exp(jnp.minimum(cum1 - col1, 0.0))
        d12 = jnp.exp(jnp.minimum(cum2 - col1, 0.0))
        d22 = jnp.exp(jnp.minimum(cum2 - col2, 0.0))
        top = dot_nt(k[:half], k)
        g22 = dot_nt(k[half:], k[half:])
        norm = jnp.concatenate(
            [
                jnp.sum(eye * top[:, :half], axis=0, keepdims=True),
                jnp.sum(eye * g22, axis=0, keepdims=True),
            ],
            axis=1,
        )
        r = lax.rsqrt(norm + EPS)
        w = rate * (r * r)
        l11 = strict * (d11 * top[:, :half]) * w[:, :half]
        l12 = d12 * top[:, half:] * w[:, half:]
        l22 = strict * (d22 * g22) * w[:, half:]
        packed = jnp.concatenate([l11, l22], axis=1)
        pair = [split(x) for x in (l11, l12, l22)]
        l_hi = [x[0] for x in pair]
        l_lo = [x[1] for x in pair]
        stage.append((l_hi, l_lo, packed, r, w, (d11, d12, d22)))
    spread = [dot(base_rows(s[2]), ones) for s in stage]
    inv = [base_inverse(x, half) for x in spread]
    lc = [jnp.concatenate([s[0][0], s[0][2]], axis=1) for s in stage]
    for mask in masks:
        mid = [dot(c * mask, expand(x)).astype(BF16) for c, x in zip(lc, inv)]
        inv = [x - dot(x, expand(z)).astype(BF16) for x, z in zip(inv, mid)]
    corner = [dot(x[:, :half], s[0][1]).astype(BF16) for s, x in zip(stage, inv)]
    corner = [(-dot(c, x[:, half:])).astype(BF16) for c, x in zip(corner, inv)]
    full = [corner_block(x[:, :half], c, x[:, half:]) for x, c in zip(inv, corner)]
    return stage, full


def solve_terms(stage, full, sides):
    lower = [(corner_block(*s[0]), corner_block(*s[1])) for s in stage]
    first = [dot(rhs.astype(BF16), x).astype(BF16) for rhs, x in zip(sides, full)]
    rest = [
        rhs - y.astype(F32) - (dot(y, l[0]) + dot(y, l[1]))
        for rhs, y, l in zip(sides, first, lower)
    ]
    return [y.astype(F32) + dot(r.astype(BF16), x) for y, r, x in zip(first, rest, full)]


def times(left, right_hi, right_lo):
    rows = left.shape[0]
    hi, lo = split(left)
    both = dot(jnp.concatenate([hi, lo], axis=0), right_hi)
    return both[:rows] + both[rows:] + dot(hi, right_lo)


def body(
    n_seq, hops, per_seq, val_total, group,
    value_hbm, beta_hbm, decay_hbm, gain_hbm, query_hbm, key_hbm, lengths_hbm, out,
    lengths, value, beta, decay, gain, query, key,
    mask_buf, ones_buf, tri_buf, rate_buf, cum_buf, live_buf, gain_buf,
    dec_buf, y_hi, y_lo, map_hi, map_lo, raw_buf, read_hi, read_lo,
    arrive, depart, val_send, val_recv, out_send, out_recv,
    load_sem, key_sem, send_sem, recv_sem,
    val_send_sem, val_recv_sem, out_send_sem, out_recv_sem,
):
    own, tokens, key_width = key.shape
    val_width = value.shape[1]
    half = tokens // 2
    me = lax.axis_index("seq")
    core = lax.axis_index("dim")
    peer = 1 - core
    base, peer_base = core * own, peer * own
    has_left, has_right = me > 0, me < n_seq - 1

    def load(source, target, index):
        return pltpu.make_async_copy(source, target, load_sem.at[index])

    def key_load(g):
        return pltpu.make_async_copy(
            key_hbm.at[pl.ds(base + g * group, group)],
            key.at[pl.ds(g * group, group)],
            key_sem.at[g],
        )

    mine, theirs = pl.ds(base, own), pl.ds(peer_base, own)
    loads = [
        load(value_hbm.at[theirs], value.at[theirs], 0),
        load(decay_hbm, decay, 1),
        load(beta_hbm, beta, 2),
        load(value_hbm.at[mine], value.at[mine], 3),
        load(gain_hbm, gain, 4),
        load(query_hbm.at[mine], query, 5),
        load(lengths_hbm, lengths, 6),
    ]
    for copy in loads[:3] + loads[6:]:
        copy.start()
    for g in range(own // group):
        key_load(g).start()
    for copy in loads[3:6]:
        copy.start()

    barrier = pltpu.get_barrier_semaphore()

    @pl.when(has_right)
    def _():
        pl.semaphore_signal(barrier, inc=1, device_id={"seq": me + 1})

    @pl.when(has_left)
    def _():
        pl.semaphore_signal(barrier, inc=1, device_id={"seq": me - 1})

    pl.semaphore_signal(barrier, inc=1, device_id={"dim": peer})

    for index, mask in enumerate(level_masks(half)):
        mask_buf[index] = mask
    for index, mask in enumerate(tri_masks(half)):
        tri_buf[index] = mask
    ones_buf[...] = block_ones(tokens)

    if hops > 1:

        @pl.when(jnp.logical_not(has_left))
        def _():
            depart[...] = jnp.zeros_like(depart)

    loads[0].wait()
    for p in range(own):
        val_send[p] = value[peer_base + p].astype(F32)
    loads[1].wait()
    loads[2].wait()
    loads[6].wait()
    position = lax.broadcasted_iota(jnp.int32, (per_seq, tokens), 1)
    for b in range(2 * own // per_seq):
        live = jnp.where(position < lengths[0, b], 1.0, 0.0)
        rows = pl.ds(b * per_seq, per_seq)
        live_buf[rows, :] = live
        rate_buf[rows, :] = beta[rows, :] * live
        cum_buf[rows, :] = decay[rows, :] * live

    pl.semaphore_wait(barrier, 1 + has_left.astype(jnp.int32) + has_right.astype(jnp.int32))

    def remote(source, target, sent, received, p, where):
        return pltpu.make_async_remote_copy(
            src_ref=source.at[p],
            dst_ref=target.at[p],
            send_sem=sent.at[p],
            recv_sem=received.at[p],
            device_id=where,
        )

    def state_copy(p):
        return remote(depart, arrive, send_sem, recv_sem, p, {"seq": me + 1})

    def value_copy(p):
        return remote(val_send, val_recv, val_send_sem, val_recv_sem, p, {"dim": peer})

    def out_copy(p):
        return remote(out_send, out_recv, out_send_sem, out_recv_sem, p, {"dim": peer})

    for p in range(own):
        value_copy(p).start()

    row = lax.broadcasted_iota(jnp.int32, (tokens, tokens), 0)
    col = lax.broadcasted_iota(jnp.int32, (tokens, tokens), 1)
    upto = jnp.where(row <= col, 1.0, 0.0)
    cum_buf[...] = jnp.dot(
        cum_buf[...], upto, precision=lax.Precision.HIGHEST, preferred_element_type=F32
    )
    loads[4].wait()
    row = lax.broadcasted_iota(jnp.int32, (val_width, val_width), 0)
    col = lax.broadcasted_iota(jnp.int32, (val_width, val_width), 1)
    gain_col = jnp.sum(jnp.where(row == col, gain[...], 0.0), axis=1, keepdims=True)
    gain_buf[...] = jnp.broadcast_to(gain_col, gain_buf.shape)
    loads[3].wait()

    def row_of(ref, p):
        return ref[pl.ds(base + p, 1), :]

    def key_phase(g, carry):
        ids = [g * group + u for u in range(group)]
        key_load(g).wait()
        items = [(key[p], row_of(rate_buf, p), row_of(cum_buf, p)) for p in ids]
        masks = [mask_buf[index] for index in range(mask_buf.shape[0])]
        tri = [tri_buf[index] for index in range(3)]
        stage, full = key_terms(items, masks, ones_buf[...], tri)
        for p, s in zip(ids, stage):
            for index, block in enumerate(s[5]):
                dec_buf[p, index] = block
        for p in ids:
            value_copy(p).wait_recv()
        sides = []
        for p, s, (k, rate, cum) in zip(ids, stage, items):
            val = jnp.concatenate([value[base + p].astype(F32), val_recv[p]], axis=0)
            kt = k.astype(F32).T
            sides.append(
                jnp.concatenate([val * (rate * s[3]), kt * (s[4] * jnp.exp(cum))], axis=0)
            )
        solved = solve_terms(stage, full, sides)
        for p, y, (k, rate, cum) in zip(ids, solved, items):
            tail = jnp.exp(cum[:, tokens - 1 :] - cum)
            t_hi, t_lo = split(y * tail)
            rows = y.shape[0]
            on_key = dot(jnp.concatenate([t_hi, t_lo], axis=0), k)
            on_key = on_key[:rows] + on_key[rows:]
            depart[p, 0] = on_key[:val_total]
            map_hi[p], map_lo[p] = split(on_key[val_total:])
            y_hi[p], y_lo[p] = split(y)

        @pl.when(jnp.logical_and(jnp.logical_not(has_left), has_right))
        def _():
            for p in ids:
                state_copy(p).start()

        return carry

    lax.fori_loop(0, own // group, key_phase, 0)
    loads[5].wait()

    def query_phase(p):
        q, k, cum = query[p], key[p], row_of(cum_buf, p)
        top = dot_nt(k[:half], q)
        g22 = dot_nt(k[half:], q[half:])
        incl = tri_buf[1]
        p11 = split(incl * (dec_buf[p, 0] * top[:, :half]))
        p12 = split(dec_buf[p, 1] * top[:, half:])
        p22 = split(incl * (dec_buf[p, 2] * g22))
        p_hi = corner_block(p11[0], p12[0], p22[0])
        p_lo = corner_block(p11[1], p12[1], p22[1])
        hi, lo = y_hi[p], y_lo[p]
        rows = hi.shape[0]
        both = dot(jnp.concatenate([hi, lo], axis=0), p_hi)
        on_query = both[:rows] + both[rows:] + dot(hi, p_lo)
        raw_buf[p] = on_query[:val_total]
        read = q.astype(F32).T * jnp.exp(cum) - on_query[val_total:]
        read_hi[p], read_lo[p] = split(read)

    def pass_on(p):
        state_copy(p).wait_recv()

        @pl.when(has_right)
        def _():
            cum = row_of(cum_buf, p)
            decayed = jnp.exp(cum[:, tokens - 1 :])
            if hops == 1:
                start = arrive[p, 0]
                moved = decayed * start - times(start, map_hi[p], map_lo[p])
                depart[p, 0] = depart[p, 0] + moved
            else:
                moving = jnp.concatenate([arrive[p, h] for h in range(hops - 1)], axis=0)
                moved = decayed * moving - times(moving, map_hi[p], map_lo[p])
                for h in range(hops - 1):
                    depart[p, h + 1] = moved[h * val_total : (h + 1) * val_total]
            state_copy(p).start()

        start = functools.reduce(jnp.add, [arrive[p, h] for h in range(hops)])
        raw_buf[p] = raw_buf[p] + times(start, read_hi[p], read_lo[p])

    def finish(p):
        raw = raw_buf[p]
        total = jnp.sum(raw * raw, axis=0, keepdims=True)
        normed = raw * (lax.rsqrt(total / val_total + EPS) * row_of(live_buf, p))
        out[base + p] = normed[:val_width] * gain_buf[...]
        out_send[p] = normed[val_width:]
        out_copy(p).start()

    def step(p, carry):
        query_phase(p)

        @pl.when(has_left)
        def _():
            pass_on(p)

        finish(p)
        return carry

    lax.fori_loop(0, own, step, 0)

    def drain(p, carry):
        @pl.when(has_right)
        def _():
            state_copy(p).wait_send()

        value_copy(p).wait_send()
        out_copy(p).wait_send()
        out_copy(p).wait_recv()
        out[peer_base + p] = out_recv[p] * gain_buf[...]
        return carry

    lax.fori_loop(0, own, drain, 0)


def solution(mesh):
    n_seq, n_dim = mesh.shape["seq"], mesh.shape["dim"]
    hops = 1 if n_seq <= WINDOW + 1 else WINDOW

    def local(query, key, value, out_gate, beta, log_decay, lengths, norm_gain):
        seqs, heads, tokens, key_width = query.shape
        val_width = value.shape[2]
        val_total = val_width * n_dim
        pairs = seqs * heads
        own = pairs // n_dim
        half = tokens // 2
        group = max(g for g in range(1, GROUP + 1) if own % g == 0)
        levels = (half // BASE).bit_length() - 1
        vmem = pl.BlockSpec(memory_space=pltpu.VMEM)
        anywhere = pl.BlockSpec(memory_space=pl.ANY)
        dma = pltpu.SemaphoreType.DMA
        flat = lambda x: x.reshape((pairs,) + x.shape[2:])
        hold = lambda x: pltpu.with_memory_space_constraint(x, pltpu.HBM)
        operands = [flat(value), flat(beta), flat(log_decay), norm_gain[None, :]]
        operands += [flat(query), flat(key), lengths.T]
        normed = pl.pallas_call(
            functools.partial(body, n_seq, hops, heads, val_total, group),
            out_shape=pltpu.VMEM((pairs, val_width, tokens), F32),
            in_specs=[anywhere] * 7,
            out_specs=vmem,
            scratch_shapes=[
                pltpu.SMEM((1, seqs), jnp.int32),
                pltpu.VMEM((pairs, val_width, tokens), BF16),
                pltpu.VMEM((pairs, tokens), F32),
                pltpu.VMEM((pairs, tokens), F32),
                pltpu.VMEM((1, val_width), F32),
                pltpu.VMEM((own, tokens, key_width), BF16),
                pltpu.VMEM((own, tokens, key_width), BF16),
                pltpu.VMEM((levels, half, tokens), BF16),
                pltpu.VMEM((tokens, tokens), BF16),
                pltpu.VMEM((3, half, half), F32),
                pltpu.VMEM((pairs, tokens), F32),
                pltpu.VMEM((pairs, tokens), F32),
                pltpu.VMEM((pairs, tokens), F32),
                pltpu.VMEM((val_width, tokens), F32),
                pltpu.VMEM((own, 3, half, half), F32),
                pltpu.VMEM((own, val_total + key_width, tokens), BF16),
                pltpu.VMEM((own, val_total + key_width, tokens), BF16),
                pltpu.VMEM((own, key_width, key_width), BF16),
                pltpu.VMEM((own, key_width, key_width), BF16),
                pltpu.VMEM((own, val_total, tokens), F32),
                pltpu.VMEM((own, key_width, tokens), BF16),
                pltpu.VMEM((own, key_width, tokens), BF16),
                pltpu.VMEM((own, hops, val_total, key_width), F32),
                pltpu.VMEM((own, hops, val_total, key_width), F32),
                pltpu.VMEM((own, val_width, tokens), F32),
                pltpu.VMEM((own, val_width, tokens), F32),
                pltpu.VMEM((own, val_width, tokens), F32),
                pltpu.VMEM((own, val_width, tokens), F32),
                dma((7,)),
                dma((own // group,)),
                dma((own,)),
                dma((own,)),
                dma((own,)),
                dma((own,)),
                dma((own,)),
                dma((own,)),
            ],
            compiler_params=pltpu.CompilerParams(
                collective_id=0, has_side_effects=True, vmem_limit_bytes=48 * 1024 * 1024
            ),
        )(*[hold(x) for x in operands])
        normed = normed.reshape(value.shape)
        gated = normed * jax.nn.silu(out_gate.astype(F32))
        return gated.astype(BF16)

    in_specs = (
        P("groups", "head", "seq", None),
        P("groups", "head", "seq", None),
        P("groups", "head", "dim", "seq"),
        P("groups", "head", "dim", "seq"),
        P("groups", "head", "seq"),
        P("groups", "head", "seq"),
        P("groups", "seq"),
        P("dim"),
    )
    out_specs = P("groups", "head", "dim", "seq")
    return jax.shard_map(local, mesh=mesh, in_specs=in_specs, out_specs=out_specs, check_vma=False)
```

```python
import functools

import jax
import jax.numpy as jnp
from jax import lax
from jax.experimental import pallas as pl
from jax.experimental.pallas import tpu as pltpu
from jax.sharding import PartitionSpec as P

WINDOW = 4
GROUP = 8
LEAD = 2
ASK = 4
PIECES = 2
BASE = 16
TILE = 8
EPS = 1e-06
F32 = jnp.float32
BF16 = jnp.bfloat16


def dot(left, right):
    return jnp.dot(left, right, preferred_element_type=F32)


def dot_nt(left, right):
    return lax.dot_general(left, right, (((1,), (1,)), ((), ())), preferred_element_type=F32)


def split(x):
    high = x.astype(BF16)
    return high, (x - high.astype(F32)).astype(BF16)


def expand(x):
    half = x.shape[0]
    zero = jnp.zeros((half, half), x.dtype)
    return jnp.concatenate(
        [
            jnp.concatenate([x[:, :half], zero], axis=1),
            jnp.concatenate([zero, x[:, half:]], axis=1),
        ],
        axis=0,
    )


def corner_block(a, b, c):
    zero = jnp.zeros((c.shape[0], a.shape[1]), c.dtype)
    return jnp.concatenate(
        [jnp.concatenate([a, b], axis=1), jnp.concatenate([zero, c], axis=1)], axis=0
    )


def level_masks(half):
    row = lax.broadcasted_iota(jnp.int32, (half, 2 * half), 0)
    col = lax.broadcasted_iota(jnp.int32, (half, 2 * half), 1)
    col = jnp.where(col >= half, col - half, col)
    differ = jnp.bitwise_xor(row, col)
    masks = []
    size = BASE
    while size < half:
        masks.append((differ >= size) & (differ < 2 * size))
        size *= 2
    return [jnp.where(m, 1.0, 0.0).astype(BF16) for m in masks]


def tri_masks(half):
    row = lax.broadcasted_iota(jnp.int32, (half, half), 0)
    col = lax.broadcasted_iota(jnp.int32, (half, half), 1)
    return [jnp.where(m, 1.0, 0.0) for m in (row < col, row <= col, row == col)]


def block_ones(tokens):
    row = lax.broadcasted_iota(jnp.int32, (tokens, tokens), 0)
    col = lax.broadcasted_iota(jnp.int32, (tokens, tokens), 1)
    return jnp.where(jnp.bitwise_xor(row, col) < BASE, 1.0, 0.0).astype(BF16)


def lane_of(rows, tokens):
    return lax.broadcasted_iota(jnp.int32, (rows, tokens), 1)


def base_rows(packed):
    half, tokens = packed.shape
    lane = lane_of(BASE, tokens)
    block = jnp.bitwise_and(lane, half - 1) // BASE
    compact = jnp.zeros((BASE, tokens), F32)
    for b in range(half // BASE):
        compact = jnp.where(block == b, packed[b * BASE : (b + 1) * BASE], compact)
    inner = jnp.bitwise_and(lane, BASE - 1)
    pieces = []
    for j in range(1, BASE):
        rows = TILE if j <= TILE else BASE
        pieces.append(jnp.where(inner[:rows] == j, compact[:rows], 0.0))
    return jnp.concatenate(pieces, axis=0).astype(BF16)


def base_inverse(spread, half):
    tokens = spread.shape[1]
    offset, place = {}, 0
    for j in range(1, BASE):
        offset[j] = place
        place += TILE if j <= TILE else BASE
    lane = jnp.bitwise_and(lane_of(TILE, tokens), BASE - 1)
    row = lax.broadcasted_iota(jnp.int32, (TILE, tokens), 0)
    top = jnp.where(lane == row, 1.0, 0.0)
    low = jnp.where(lane == row + TILE, 1.0, 0.0)
    for j in range(BASE - 1, 0, -1):
        at = offset[j]
        if j > TILE:
            line = low[j - TILE : j - TILE + 1]
            low = low - spread[at + TILE : at + BASE] * line
        else:
            line = low[:1] if j == TILE else top[j : j + 1]
        top = top - spread[at : at + TILE] * line
    found = jnp.concatenate([top, low], axis=0)
    lane = lane_of(BASE, tokens)
    block = jnp.bitwise_and(lane, half - 1) // BASE
    return jnp.concatenate(
        [jnp.where(block == b, found, 0.0) for b in range(half // BASE)], axis=0
    ).astype(BF16)


def key_terms(items, masks, ones, tri):
    strict, _, eye = tri
    tokens = items[0][0].shape[0]
    half = tokens // 2
    stage = []
    for k, rate, cum in items:
        cum1, cum2 = cum[:, :half], cum[:, half:]
        col1 = jnp.sum(eye * cum1, axis=1, keepdims=True)
        col2 = jnp.sum(eye * cum2, axis=1, keepdims=True)
        d11 = jnp.exp(jnp.minimum(cum1 - col1, 0.0))
        d12 = jnp.exp(jnp.minimum(cum2 - col1, 0.0))
        d22 = jnp.exp(jnp.minimum(cum2 - col2, 0.0))
        top = dot_nt(k[:half], k)
        g22 = dot_nt(k[half:], k[half:])
        norm = jnp.concatenate(
            [
                jnp.sum(eye * top[:, :half], axis=0, keepdims=True),
                jnp.sum(eye * g22, axis=0, keepdims=True),
            ],
            axis=1,
        )
        r = lax.rsqrt(norm + EPS)
        w = rate * (r * r)
        l11 = strict * (d11 * top[:, :half]) * w[:, :half]
        l12 = d12 * top[:, half:] * w[:, half:]
        l22 = strict * (d22 * g22) * w[:, half:]
        packed = jnp.concatenate([l11, l22], axis=1)
        pair = [split(x) for x in (l11, l12, l22)]
        l_hi = [x[0] for x in pair]
        l_lo = [x[1] for x in pair]
        stage.append((l_hi, l_lo, packed, r, w, (d11, d12, d22)))
    spread = [dot(base_rows(s[2]), ones) for s in stage]
    inv = [base_inverse(x, half) for x in spread]
    lc = [jnp.concatenate([s[0][0], s[0][2]], axis=1) for s in stage]
    for mask in masks:
        mid = [dot(x, expand(c * mask)).astype(BF16) for c, x in zip(lc, inv)]
        inv = [x - dot(z, expand(x)).astype(BF16) for x, z in zip(inv, mid)]
    corner = [dot(x[:, :half], s[0][1]).astype(BF16) for s, x in zip(stage, inv)]
    corner = [(-dot(c, x[:, half:])).astype(BF16) for c, x in zip(corner, inv)]
    full = [corner_block(x[:, :half], c, x[:, half:]) for x, c in zip(inv, corner)]
    return stage, full


def solve_terms(stage, full, sides):
    lower = [(corner_block(*s[0]), corner_block(*s[1])) for s in stage]
    first = [dot(rhs.astype(BF16), x).astype(BF16) for rhs, x in zip(sides, full)]
    rest = [
        rhs - y.astype(F32) - (dot(y, l[0]) + dot(y, l[1]))
        for rhs, y, l in zip(sides, first, lower)
    ]
    return [y.astype(F32) + dot(r.astype(BF16), x) for y, r, x in zip(first, rest, full)]


def times(left, right_hi, right_lo):
    rows = left.shape[0]
    hi, lo = split(left)
    both = dot(jnp.concatenate([hi, lo], axis=0), right_hi)
    return both[:rows] + both[rows:] + dot(hi, right_lo)


def body(
    n_seq, hops, per_seq, val_total, group, lead, ask,
    value_hbm, beta_hbm, decay_hbm, gain_hbm, query_hbm, key_hbm, lengths_hbm, out,
    lengths, value, beta, decay, gain, query, key,
    mask_buf, ones_buf, tri_buf, rate_buf, cum_buf, live_buf, gain_buf,
    dec_buf, y_hi, y_lo, map_hi, map_lo, raw_buf, read_hi, read_lo,
    arrive, depart, val_send, val_recv, out_send, out_recv,
    load_sem, key_sem, send_sem, recv_sem,
    val_send_sem, val_recv_sem, out_send_sem, out_recv_sem,
):
    own, tokens, key_width = key.shape
    val_width = value.shape[1]
    half = tokens // 2
    me = lax.axis_index("seq")
    core = lax.axis_index("dim")
    peer = 1 - core
    base, peer_base = core * own, peer * own
    has_left, has_right = me > 0, me < n_seq - 1

    def load(source, target, index):
        return pltpu.make_async_copy(source, target, load_sem.at[index])

    def key_load(g):
        return pltpu.make_async_copy(
            key_hbm.at[pl.ds(base + g * lead, lead)],
            key.at[pl.ds(g * lead, lead)],
            key_sem.at[g],
        )

    mine, theirs = pl.ds(base, own), pl.ds(peer_base, own)
    loads = [
        load(value_hbm.at[theirs], value.at[theirs], 0),
        load(decay_hbm, decay, 1),
        load(beta_hbm, beta, 2),
        load(value_hbm.at[mine], value.at[mine], 3),
        load(gain_hbm, gain, 4),
        load(query_hbm.at[mine], query, 5),
        load(lengths_hbm, lengths, 6),
    ]
    key_load(0).start()
    for copy in loads[:3] + loads[6:]:
        copy.start()
    for g in range(1, own // lead):
        key_load(g).start()
    for copy in loads[3:6]:
        copy.start()

    barrier = pltpu.get_barrier_semaphore()

    @pl.when(has_right)
    def _():
        pl.semaphore_signal(barrier, inc=1, device_id={"seq": me + 1})

    @pl.when(has_left)
    def _():
        pl.semaphore_signal(barrier, inc=1, device_id={"seq": me - 1})

    pl.semaphore_signal(barrier, inc=1, device_id={"dim": peer})

    for index, mask in enumerate(level_masks(half)):
        mask_buf[index] = mask
    for index, mask in enumerate(tri_masks(half)):
        tri_buf[index] = mask
    ones_buf[...] = block_ones(tokens)

    if hops > 1:

        @pl.when(jnp.logical_not(has_left))
        def _():
            depart[...] = jnp.zeros_like(depart)

    loads[1].wait()
    loads[2].wait()
    loads[6].wait()
    position = lax.broadcasted_iota(jnp.int32, (per_seq, tokens), 1)
    steps = []
    for b in range(2 * own // per_seq):
        live = jnp.where(position < lengths[0, b], 1.0, 0.0)
        rows = pl.ds(b * per_seq, per_seq)
        live_buf[rows, :] = live
        rate_buf[rows, :] = beta[rows, :] * live
        steps.append(decay[rows, :] * live)
    steps = jnp.concatenate(steps, axis=0)
    high, low = split(steps)
    rest = (steps - high.astype(F32) - low.astype(F32)).astype(BF16)
    row = lax.broadcasted_iota(jnp.int32, (tokens, tokens), 0)
    col = lax.broadcasted_iota(jnp.int32, (tokens, tokens), 1)
    upto = jnp.where(row <= col, 1.0, 0.0).astype(BF16)
    cum_buf[...] = dot(high, upto) + dot(low, upto) + dot(rest, upto)

    loads[0].wait()
    for p in range(own):
        val_send[p] = value[peer_base + p].astype(F32)

    pl.semaphore_wait(barrier, 1 + has_left.astype(jnp.int32) + has_right.astype(jnp.int32))

    def state_copy(p, h):
        return pltpu.make_async_remote_copy(
            src_ref=depart.at[p, h],
            dst_ref=arrive.at[p, h],
            send_sem=send_sem.at[p, h],
            recv_sem=recv_sem.at[p, h],
            device_id={"seq": me + 1},
        )

    def remote(source, target, sent, received, p, where):
        return pltpu.make_async_remote_copy(
            src_ref=source.at[p],
            dst_ref=target.at[p],
            send_sem=sent.at[p],
            recv_sem=received.at[p],
            device_id=where,
        )

    def value_copy(p):
        return remote(val_send, val_recv, val_send_sem, val_recv_sem, p, {"dim": peer})

    def out_copy(p):
        return remote(out_send, out_recv, out_send_sem, out_recv_sem, p, {"dim": peer})

    for p in range(own):
        value_copy(p).start()

    loads[3].wait()

    def row_of(ref, p):
        return ref[pl.ds(base + p, 1), :]

    piece = val_total // PIECES

    def key_phase(first, size, g, carry):
        ids = [g * size + u for u in range(size)]
        for u in range(size // lead):
            key_load(g * (size // lead) + u).wait()
        items = [(key[p], row_of(rate_buf, p), row_of(cum_buf, p)) for p in ids]
        masks = [mask_buf[index] for index in range(mask_buf.shape[0])]
        tri = [tri_buf[index] for index in range(3)]
        stage, full = key_terms(items, masks, ones_buf[...], tri)
        for p, s in zip(ids, stage):
            for index, block in enumerate(s[5]):
                dec_buf[p, index] = block
        for p in ids:
            value_copy(p).wait_recv()
        sides = []
        for p, s, (k, rate, cum) in zip(ids, stage, items):
            val = jnp.concatenate([value[base + p].astype(F32), val_recv[p]], axis=0)
            side = val * (rate * s[3])
            if not first:
                kt = k.astype(F32).T
                side = jnp.concatenate([side, kt * (s[4] * jnp.exp(cum))], axis=0)
            sides.append(side)
        solved = solve_terms(stage, full, sides)
        for p, y, (k, rate, cum) in zip(ids, solved, items):
            tail = jnp.exp(cum[:, tokens - 1 :] - cum)
            t_hi, t_lo = split(y * tail)
            on_key = dot(t_hi, k) + dot(t_lo, k)
            for h in range(PIECES):
                depart[p, h, 0] = on_key[h * piece : (h + 1) * piece]
            if not first:
                map_hi[p], map_lo[p] = split(on_key[val_total:])
            rows = pl.ds(0, y.shape[0])
            y_hi[p, rows], y_lo[p, rows] = split(y)
        if first:
            for p in ids:
                for h in range(PIECES):
                    state_copy(p, h).start()
        return carry

    @pl.when(jnp.logical_not(has_left))
    def _():
        lax.fori_loop(0, own // lead, functools.partial(key_phase, True, lead), 0)

    @pl.when(has_left)
    def _():
        lax.fori_loop(0, own // group, functools.partial(key_phase, False, group), 0)

    loads[4].wait()
    row = lax.broadcasted_iota(jnp.int32, (val_width, val_width), 0)
    col = lax.broadcasted_iota(jnp.int32, (val_width, val_width), 1)
    gain_col = jnp.sum(jnp.where(row == col, gain[...], 0.0), axis=1, keepdims=True)
    gain_buf[...] = jnp.broadcast_to(gain_col, gain_buf.shape)
    loads[5].wait()

    def query_phase(first, size, g, carry):
        ids = [g * size + u for u in range(size)]
        incl = tri_buf[1]
        tops = [dot_nt(key[p, :half], query[p]) for p in ids]
        lows = [dot_nt(key[p, half:], query[p, half:]) for p in ids]
        parts = []
        for p, top, low in zip(ids, tops, lows):
            p11 = split(incl * (dec_buf[p, 0] * top[:, :half]))
            p12 = split(dec_buf[p, 1] * top[:, half:])
            p22 = split(incl * (dec_buf[p, 2] * low))
            parts.append([corner_block(p11[n], p12[n], p22[n]) for n in range(2)])
        rows = pl.ds(0, val_total if first else val_total + key_width)
        for p, (p_hi, p_lo) in zip(ids, parts):
            hi, lo = y_hi[p, rows], y_lo[p, rows]
            on_query = dot(hi, p_hi) + dot(lo, p_hi) + dot(hi, p_lo)
            raw_buf[p] = on_query[:val_total]
            if not first:
                cum = row_of(cum_buf, p)
                read = query[p].astype(F32).T * jnp.exp(cum) - on_query[val_total:]
                read_hi[p], read_lo[p] = split(read)
        return carry

    def pass_on(p, h):
        state_copy(p, h).wait_recv()

        @pl.when(has_right)
        def _():
            cum = row_of(cum_buf, p)
            decayed = jnp.exp(cum[:, tokens - 1 :])
            if hops == 1:
                start = arrive[p, h, 0]
                moved = decayed * start - times(start, map_hi[p], map_lo[p])
                depart[p, h, 0] = depart[p, h, 0] + moved
            else:
                moving = jnp.concatenate([arrive[p, h, n] for n in range(hops - 1)], axis=0)
                moved = decayed * moving - times(moving, map_hi[p], map_lo[p])
                for n in range(hops - 1):
                    depart[p, h, n + 1] = moved[n * piece : (n + 1) * piece]
            state_copy(p, h).start()

    def read_out(p):
        starts = [
            functools.reduce(jnp.add, [arrive[p, h, n] for n in range(hops)])
            for h in range(PIECES)
        ]
        start = jnp.concatenate(starts, axis=0)
        raw_buf[p] = raw_buf[p] + times(start, read_hi[p], read_lo[p])

    def finish(p):
        raw = raw_buf[p]
        total = jnp.sum(raw * raw, axis=0, keepdims=True)
        normed = raw * (lax.rsqrt(total / val_total + EPS) * row_of(live_buf, p))
        out[base + p] = normed[:val_width] * gain_buf[...]
        out_send[p] = normed[val_width:]
        out_copy(p).start()

    def passing(p, carry):
        for h in range(PIECES):
            pass_on(p, h)
        return carry

    def ending(p, carry):
        read_out(p)
        finish(p)
        return carry

    def both(p, carry):
        passing(p, carry)
        return ending(p, carry)

    def lone(p, carry):
        finish(p)
        return carry

    batch = functools.partial(query_phase, False, ask)

    @pl.when(jnp.logical_not(has_left))
    def _():
        lax.fori_loop(0, own // ask, functools.partial(query_phase, True, ask), 0)
        lax.fori_loop(0, own, lone, 0)

    @pl.when(has_left)
    def _():
        early = me == 1
        lax.fori_loop(0, jnp.where(early, own, 0), passing, 0)
        lax.fori_loop(0, own // ask, batch, 0)

        @pl.when(early)
        def _():
            lax.fori_loop(0, own, ending, 0)

        @pl.when(jnp.logical_not(early))
        def _():
            lax.fori_loop(0, own, both, 0)

    def drain(p, carry):
        @pl.when(has_right)
        def _():
            for h in range(PIECES):
                state_copy(p, h).wait_send()

        value_copy(p).wait_send()
        out_copy(p).wait_send()
        out_copy(p).wait_recv()
        out[peer_base + p] = out_recv[p] * gain_buf[...]
        return carry

    lax.fori_loop(0, own, drain, 0)


def solution(mesh):
    n_seq, n_dim = mesh.shape["seq"], mesh.shape["dim"]
    hops = 1 if n_seq <= WINDOW + 1 else WINDOW

    def local(query, key, value, out_gate, beta, log_decay, lengths, norm_gain):
        seqs, heads, tokens, key_width = query.shape
        val_width = value.shape[2]
        val_total = val_width * n_dim
        pairs = seqs * heads
        own = pairs // n_dim
        half = tokens // 2
        group = max(g for g in range(1, GROUP + 1) if own % g == 0)
        lead = max(g for g in range(1, LEAD + 1) if group % g == 0)
        ask = max(g for g in range(1, ASK + 1) if own % g == 0)
        levels = (half // BASE).bit_length() - 1
        vmem = pl.BlockSpec(memory_space=pltpu.VMEM)
        anywhere = pl.BlockSpec(memory_space=pl.ANY)
        dma = pltpu.SemaphoreType.DMA
        flat = lambda x: x.reshape((pairs,) + x.shape[2:])
        hold = lambda x: pltpu.with_memory_space_constraint(x, pltpu.HBM)
        operands = [flat(value), flat(beta), flat(log_decay), norm_gain[None, :]]
        operands += [flat(query), flat(key), lengths.T]
        normed = pl.pallas_call(
            functools.partial(body, n_seq, hops, heads, val_total, group, lead, ask),
            out_shape=pltpu.VMEM((pairs, val_width, tokens), F32),
            in_specs=[anywhere] * 7,
            out_specs=vmem,
            scratch_shapes=[
                pltpu.SMEM((1, seqs), jnp.int32),
                pltpu.VMEM((pairs, val_width, tokens), BF16),
                pltpu.VMEM((pairs, tokens), F32),
                pltpu.VMEM((pairs, tokens), F32),
                pltpu.VMEM((1, val_width), F32),
                pltpu.VMEM((own, tokens, key_width), BF16),
                pltpu.VMEM((own, tokens, key_width), BF16),
                pltpu.VMEM((levels, half, tokens), BF16),
                pltpu.VMEM((tokens, tokens), BF16),
                pltpu.VMEM((3, half, half), F32),
                pltpu.VMEM((pairs, tokens), F32),
                pltpu.VMEM((pairs, tokens), F32),
                pltpu.VMEM((pairs, tokens), F32),
                pltpu.VMEM((val_width, tokens), F32),
                pltpu.VMEM((own, 3, half, half), F32),
                pltpu.VMEM((own, val_total + key_width, tokens), BF16),
                pltpu.VMEM((own, val_total + key_width, tokens), BF16),
                pltpu.VMEM((own, key_width, key_width), BF16),
                pltpu.VMEM((own, key_width, key_width), BF16),
                pltpu.VMEM((own, val_total, tokens), F32),
                pltpu.VMEM((own, key_width, tokens), BF16),
                pltpu.VMEM((own, key_width, tokens), BF16),
                pltpu.VMEM((own, PIECES, hops, val_total // PIECES, key_width), F32),
                pltpu.VMEM((own, PIECES, hops, val_total // PIECES, key_width), F32),
                pltpu.VMEM((own, val_width, tokens), F32),
                pltpu.VMEM((own, val_width, tokens), F32),
                pltpu.VMEM((own, val_width, tokens), F32),
                pltpu.VMEM((own, val_width, tokens), F32),
                dma((7,)),
                dma((own // lead,)),
                dma((own, PIECES)),
                dma((own, PIECES)),
                dma((own,)),
                dma((own,)),
                dma((own,)),
                dma((own,)),
            ],
            compiler_params=pltpu.CompilerParams(
                collective_id=0, has_side_effects=True, vmem_limit_bytes=48 * 1024 * 1024
            ),
        )(*[hold(x) for x in operands])
        normed = normed.reshape(value.shape)
        gated = normed * jax.nn.silu(out_gate.astype(F32))
        return gated.astype(BF16)

    in_specs = (
        P("groups", "head", "seq", None),
        P("groups", "head", "seq", None),
        P("groups", "head", "dim", "seq"),
        P("groups", "head", "dim", "seq"),
        P("groups", "head", "seq"),
        P("groups", "head", "seq"),
        P("groups", "seq"),
        P("dim"),
    )
    out_specs = P("groups", "head", "dim", "seq")
    return jax.shard_map(local, mesh=mesh, in_specs=in_specs, out_specs=out_specs, check_vma=False)
```

```python
import functools

import jax
import jax.numpy as jnp
from jax import lax
from jax.experimental import pallas as pl
from jax.experimental.pallas import tpu as pltpu
from jax.sharding import PartitionSpec as P

WINDOW = 4
GROUP = 8
LEAD = 2
ASK = 4
PIECES = 2
BASE = 16
TILE = 8
EPS = 1e-06
F32 = jnp.float32
BF16 = jnp.bfloat16


def dot(left, right):
    return jnp.dot(left, right, preferred_element_type=F32)


def dot_nt(left, right):
    return lax.dot_general(left, right, (((1,), (1,)), ((), ())), preferred_element_type=F32)


def split(x):
    high = x.astype(BF16)
    return high, (x - high.astype(F32)).astype(BF16)


def expand(x):
    half = x.shape[0]
    zero = jnp.zeros((half, half), x.dtype)
    return jnp.concatenate(
        [
            jnp.concatenate([x[:, :half], zero], axis=1),
            jnp.concatenate([zero, x[:, half:]], axis=1),
        ],
        axis=0,
    )


def corner_block(a, b, c):
    zero = jnp.zeros((c.shape[0], a.shape[1]), c.dtype)
    return jnp.concatenate(
        [jnp.concatenate([a, b], axis=1), jnp.concatenate([zero, c], axis=1)], axis=0
    )


def level_masks(half):
    row = lax.broadcasted_iota(jnp.int32, (half, 2 * half), 0)
    col = lax.broadcasted_iota(jnp.int32, (half, 2 * half), 1)
    col = jnp.where(col >= half, col - half, col)
    differ = jnp.bitwise_xor(row, col)
    masks = []
    size = BASE
    while size < half:
        masks.append((differ >= size) & (differ < 2 * size))
        size *= 2
    return [jnp.where(m, 1.0, 0.0).astype(BF16) for m in masks]


def tri_masks(half):
    row = lax.broadcasted_iota(jnp.int32, (half, half), 0)
    col = lax.broadcasted_iota(jnp.int32, (half, half), 1)
    return [jnp.where(m, 1.0, 0.0) for m in (row < col, row <= col, row == col)]


def block_ones(tokens):
    row = lax.broadcasted_iota(jnp.int32, (tokens, tokens), 0)
    col = lax.broadcasted_iota(jnp.int32, (tokens, tokens), 1)
    return jnp.where(jnp.bitwise_xor(row, col) < BASE, 1.0, 0.0).astype(BF16)


def lane_of(rows, tokens):
    return lax.broadcasted_iota(jnp.int32, (rows, tokens), 1)


def base_rows(packed):
    half, tokens = packed.shape
    lane = lane_of(BASE, tokens)
    block = jnp.bitwise_and(lane, half - 1) // BASE
    compact = jnp.zeros((BASE, tokens), F32)
    for b in range(half // BASE):
        compact = jnp.where(block == b, packed[b * BASE : (b + 1) * BASE], compact)
    inner = jnp.bitwise_and(lane, BASE - 1)
    pieces = []
    for j in range(1, BASE):
        rows = TILE if j <= TILE else BASE
        pieces.append(jnp.where(inner[:rows] == j, compact[:rows], 0.0))
    return jnp.concatenate(pieces, axis=0).astype(BF16)


def base_inverse(spread, half):
    tokens = spread.shape[1]
    offset, place = {}, 0
    for j in range(1, BASE):
        offset[j] = place
        place += TILE if j <= TILE else BASE
    lane = jnp.bitwise_and(lane_of(TILE, tokens), BASE - 1)
    row = lax.broadcasted_iota(jnp.int32, (TILE, tokens), 0)
    top = jnp.where(lane == row, 1.0, 0.0)
    low = jnp.where(lane == row + TILE, 1.0, 0.0)
    for j in range(BASE - 1, 0, -1):
        at = offset[j]
        if j > TILE:
            line = low[j - TILE : j - TILE + 1]
            low = low - spread[at + TILE : at + BASE] * line
        else:
            line = low[:1] if j == TILE else top[j : j + 1]
        top = top - spread[at : at + TILE] * line
    found = jnp.concatenate([top, low], axis=0)
    lane = lane_of(BASE, tokens)
    block = jnp.bitwise_and(lane, half - 1) // BASE
    return jnp.concatenate(
        [jnp.where(block == b, found, 0.0) for b in range(half // BASE)], axis=0
    ).astype(BF16)


def decays(cum, eye, keep):
    half = eye.shape[0]
    cum1, cum2 = cum[:, :half], cum[:, half:]
    col1 = jnp.sum(eye * cum1, axis=1, keepdims=True)
    col2 = jnp.sum(eye * cum2, axis=1, keepdims=True)
    return (
        jnp.where(keep > 0.0, jnp.exp(cum1 - col1), 0.0),
        jnp.exp(cum2 - col1),
        jnp.where(keep > 0.0, jnp.exp(cum2 - col2), 0.0),
    )


def key_terms(items, masks, ones, tri):
    strict, _, eye = tri
    tokens = items[0][0].shape[0]
    half = tokens // 2
    stage = []
    for k, rate, cum in items:
        d11, d12, d22 = decays(cum, eye, strict)
        top = dot_nt(k[:half], k)
        g22 = dot_nt(k[half:], k[half:])
        norm = jnp.concatenate(
            [
                jnp.sum(eye * top[:, :half], axis=0, keepdims=True),
                jnp.sum(eye * g22, axis=0, keepdims=True),
            ],
            axis=1,
        )
        r = lax.rsqrt(norm + EPS)
        w = rate * (r * r)
        l11 = d11 * top[:, :half] * w[:, :half]
        l12 = d12 * top[:, half:] * w[:, half:]
        l22 = d22 * g22 * w[:, half:]
        packed = jnp.concatenate([l11, l22], axis=1)
        pair = [split(x) for x in (l11 + eye, l12, l22 + eye)]
        l_hi = [x[0] for x in pair]
        l_lo = [x[1] for x in pair]
        stage.append((l_hi, l_lo, packed, r, w))
    spread = [dot(base_rows(s[2]), ones) for s in stage]
    inv = [base_inverse(x, half) for x in spread]
    lc = [jnp.concatenate([s[0][0], s[0][2]], axis=1) for s in stage]
    for mask in masks:
        mid = [dot(x, expand(c * mask)).astype(BF16) for c, x in zip(lc, inv)]
        inv = [x - dot(z, expand(x)).astype(BF16) for x, z in zip(inv, mid)]
    corner = [dot(x[:, :half], s[0][1]).astype(BF16) for s, x in zip(stage, inv)]
    corner = [(-dot(c, x[:, half:])).astype(BF16) for c, x in zip(corner, inv)]
    full = [corner_block(x[:, :half], c, x[:, half:]) for x, c in zip(inv, corner)]
    return stage, full


def solve_terms(stage, full, sides):
    lower = [(corner_block(*s[0]), corner_block(*s[1])) for s in stage]
    first = [dot(rhs.astype(BF16), x).astype(BF16) for rhs, x in zip(sides, full)]
    rest = [
        rhs - (dot(y, l[0]) + dot(y, l[1]))
        for rhs, y, l in zip(sides, first, lower)
    ]
    return [y.astype(F32) + dot(r.astype(BF16), x) for y, r, x in zip(first, rest, full)]


def times(left, right_hi, right_lo):
    rows = left.shape[0]
    hi, lo = split(left)
    both = dot(jnp.concatenate([hi, lo], axis=0), right_hi)
    return both[:rows] + both[rows:] + dot(hi, right_lo)


def body(
    n_seq, hops, per_seq, val_total, group, lead, ask,
    value_hbm, beta_hbm, decay_hbm, gain_hbm, query_hbm, key_hbm, lengths_hbm, out,
    lengths, value, beta, decay, gain, query, key,
    mask_buf, ones_buf, tri_buf, rate_buf, cum_buf, live_buf, gain_buf,
    y_buf, map_hi, map_lo, raw_buf, read_hi, read_lo,
    arrive, depart, val_send, val_recv, out_send, out_recv,
    load_sem, key_sem, send_sem, recv_sem,
    val_send_sem, val_recv_sem, out_send_sem, out_recv_sem,
):
    own, tokens, key_width = key.shape
    val_width = value.shape[1]
    half = tokens // 2
    me = lax.axis_index("seq")
    core = lax.axis_index("dim")
    peer = 1 - core
    base, peer_base = core * own, peer * own
    has_left, has_right = me > 0, me < n_seq - 1

    def load(source, target, index):
        return pltpu.make_async_copy(source, target, load_sem.at[index])

    def key_load(g):
        return pltpu.make_async_copy(
            key_hbm.at[pl.ds(base + g * lead, lead)],
            key.at[pl.ds(g * lead, lead)],
            key_sem.at[g],
        )

    mine, theirs = pl.ds(base, own), pl.ds(peer_base, own)
    loads = [
        load(value_hbm.at[theirs], value.at[theirs], 0),
        load(decay_hbm, decay, 1),
        load(beta_hbm, beta, 2),
        load(value_hbm.at[mine], value.at[mine], 3),
        load(gain_hbm, gain, 4),
        load(query_hbm.at[mine], query, 5),
        load(lengths_hbm, lengths, 6),
    ]
    key_load(0).start()
    for copy in loads[:3] + loads[6:]:
        copy.start()
    for g in range(1, own // lead):
        key_load(g).start()
    for copy in loads[3:6]:
        copy.start()

    barrier = pltpu.get_barrier_semaphore()

    @pl.when(has_right)
    def _():
        pl.semaphore_signal(barrier, inc=1, device_id={"seq": me + 1})

    @pl.when(has_left)
    def _():
        pl.semaphore_signal(barrier, inc=1, device_id={"seq": me - 1})

    pl.semaphore_signal(barrier, inc=1, device_id={"dim": peer})

    for index, mask in enumerate(level_masks(half)):
        mask_buf[index] = mask
    for index, mask in enumerate(tri_masks(half)):
        tri_buf[index] = mask
    ones_buf[...] = block_ones(tokens)

    if hops > 1:

        @pl.when(jnp.logical_not(has_left))
        def _():
            depart[...] = jnp.zeros_like(depart)

    loads[1].wait()
    loads[2].wait()
    loads[6].wait()
    position = lax.broadcasted_iota(jnp.int32, (per_seq, tokens), 1)
    steps = []
    for b in range(2 * own // per_seq):
        live = jnp.where(position < lengths[0, b], 1.0, 0.0)
        rows = pl.ds(b * per_seq, per_seq)
        live_buf[rows, :] = live
        rate_buf[rows, :] = beta[rows, :] * live
        steps.append(decay[rows, :] * live)
    steps = jnp.concatenate(steps, axis=0)
    high, low = split(steps)
    rest = (steps - high.astype(F32) - low.astype(F32)).astype(BF16)
    row = lax.broadcasted_iota(jnp.int32, (tokens, tokens), 0)
    col = lax.broadcasted_iota(jnp.int32, (tokens, tokens), 1)
    upto = jnp.where(row <= col, 1.0, 0.0).astype(BF16)
    cum_buf[...] = dot(high, upto) + dot(low, upto) + dot(rest, upto)

    loads[0].wait()
    for p in range(own):
        val_send[p] = value[peer_base + p].astype(F32)

    pl.semaphore_wait(barrier, 1 + has_left.astype(jnp.int32) + has_right.astype(jnp.int32))

    def state_copy(p, h):
        return pltpu.make_async_remote_copy(
            src_ref=depart.at[p, h],
            dst_ref=arrive.at[p, h],
            send_sem=send_sem.at[p, h],
            recv_sem=recv_sem.at[p, h],
            device_id={"seq": me + 1},
        )

    def remote(source, target, sent, received, p, where):
        return pltpu.make_async_remote_copy(
            src_ref=source.at[p],
            dst_ref=target.at[p],
            send_sem=sent.at[p],
            recv_sem=received.at[p],
            device_id=where,
        )

    def value_copy(p):
        return remote(val_send, val_recv, val_send_sem, val_recv_sem, p, {"dim": peer})

    def out_copy(p):
        return remote(out_send, out_recv, out_send_sem, out_recv_sem, p, {"dim": peer})

    for p in range(own):
        value_copy(p).start()

    loads[3].wait()

    def row_of(ref, p):
        return ref[pl.ds(base + p, 1), :]

    piece = val_total // PIECES
    assert piece == val_width

    def key_phase(first, size, g, carry):
        ids = [g * size + u for u in range(size)]
        for u in range(size // lead):
            key_load(g * (size // lead) + u).wait()
        items = [(key[p], row_of(rate_buf, p), row_of(cum_buf, p)) for p in ids]
        masks = [mask_buf[index] for index in range(mask_buf.shape[0])]
        tri = [tri_buf[index] for index in range(3)]
        stage, full = key_terms(items, masks, ones_buf[...], tri)
        if first:
            tails = [jnp.exp(cum[:, tokens - 1 :] - cum) for k, rate, cum in items]
            for h in range(PIECES):
                if h > 0:
                    for p in ids:
                        value_copy(p).wait_recv()
                parts = [val_recv[p] if h else value[base + p].astype(F32) for p in ids]
                sides = [v * (rate * s[3]) for v, s, (k, rate, cum) in zip(parts, stage, items)]
                solved = solve_terms(stage, full, sides)
                for p, y, tail, (k, rate, cum) in zip(ids, solved, tails, items):
                    t_hi, t_lo = split(y * tail)
                    depart[p, h, 0] = dot(t_hi, k) + dot(t_lo, k)
                for p in ids:
                    state_copy(p, h).start()
                for p, y in zip(ids, solved):
                    y_buf[p, pl.ds(h * piece, piece)] = y
        else:
            for p in ids:
                value_copy(p).wait_recv()
            sides = []
            for p, s, (k, rate, cum) in zip(ids, stage, items):
                val = jnp.concatenate([value[base + p].astype(F32), val_recv[p]], axis=0)
                side = val * (rate * s[3])
                if not first:
                    kt = k.astype(F32).T
                    side = jnp.concatenate([side, kt * (s[4] * jnp.exp(cum))], axis=0)
                sides.append(side)
            solved = solve_terms(stage, full, sides)
            for p, y, (k, rate, cum) in zip(ids, solved, items):
                tail = jnp.exp(cum[:, tokens - 1 :] - cum)
                t_hi, t_lo = split(y * tail)
                on_key = dot(t_hi, k) + dot(t_lo, k)
                for h in range(PIECES):
                    depart[p, h, 0] = on_key[h * piece : (h + 1) * piece]
                if not first:
                    map_hi[p], map_lo[p] = split(on_key[val_total:])
                y_buf[p, pl.ds(0, y.shape[0])] = y
        return carry

    @pl.when(jnp.logical_not(has_left))
    def _():
        lax.fori_loop(0, own // lead, functools.partial(key_phase, True, lead), 0)

    @pl.when(has_left)
    def _():
        lax.fori_loop(0, own // group, functools.partial(key_phase, False, group), 0)

    for p in range(own):
        value_copy(p).wait_send()
    loads[4].wait()
    row = lax.broadcasted_iota(jnp.int32, (val_width, val_width), 0)
    col = lax.broadcasted_iota(jnp.int32, (val_width, val_width), 1)
    gain_col = jnp.sum(jnp.where(row == col, gain[...], 0.0), axis=1, keepdims=True)
    gain_buf[...] = jnp.broadcast_to(gain_col, gain_buf.shape)
    loads[5].wait()

    def query_phase(first, size, g, carry):
        ids = [g * size + u for u in range(size)]
        incl = tri_buf[1]
        tops = [dot_nt(key[p, :half], query[p]) for p in ids]
        lows = [dot_nt(key[p, half:], query[p, half:]) for p in ids]
        parts = []
        for p, top, low in zip(ids, tops, lows):
            d11, d12, d22 = decays(row_of(cum_buf, p), tri_buf[2], incl)
            p11 = split(d11 * top[:, :half])
            p12 = split(d12 * top[:, half:])
            p22 = split(d22 * low)
            parts.append([corner_block(p11[n], p12[n], p22[n]) for n in range(2)])
        rows = pl.ds(0, val_total if first else val_total + key_width)
        for p, (p_hi, p_lo) in zip(ids, parts):
            hi, lo = split(y_buf[p, rows])
            on_query = dot(hi, p_hi) + dot(lo, p_hi) + dot(hi, p_lo)
            raw_buf[p] = on_query[:val_total]
            if not first:
                cum = row_of(cum_buf, p)
                read = query[p].astype(F32).T * jnp.exp(cum) - on_query[val_total:]
                read_hi[p], read_lo[p] = split(read)
        return carry

    def pass_on(p, h):
        state_copy(p, h).wait_recv()

        @pl.when(has_right)
        def _():
            cum = row_of(cum_buf, p)
            decayed = jnp.exp(cum[:, tokens - 1 :])
            if hops == 1:
                start = arrive[p, h, 0]
                moved = decayed * start - times(start, map_hi[p], map_lo[p])
                depart[p, h, 0] = depart[p, h, 0] + moved
            else:
                moving = jnp.concatenate([arrive[p, h, n] for n in range(hops - 1)], axis=0)
                moved = decayed * moving - times(moving, map_hi[p], map_lo[p])
                for n in range(hops - 1):
                    depart[p, h, n + 1] = moved[n * piece : (n + 1) * piece]
            state_copy(p, h).start()

    def read_out(p):
        starts = [
            functools.reduce(jnp.add, [arrive[p, h, n] for n in range(hops)])
            for h in range(PIECES)
        ]
        start = jnp.concatenate(starts, axis=0)
        raw_buf[p] = raw_buf[p] + times(start, read_hi[p], read_lo[p])

    def finish(p):
        raw = raw_buf[p]
        total = jnp.sum(raw * raw, axis=0, keepdims=True)
        normed = raw * (lax.rsqrt(total / val_total + EPS) * row_of(live_buf, p))
        out[base + p] = normed[:val_width] * gain_buf[...]
        out_send[p] = normed[val_width:]
        out_copy(p).start()

    def passing(p, carry):
        for h in range(PIECES):
            pass_on(p, h)
        return carry

    def ending(p, carry):
        read_out(p)
        finish(p)
        return carry

    def both(p, carry):
        passing(p, carry)
        return ending(p, carry)

    def lone(p, carry):
        finish(p)
        return carry

    batch = functools.partial(query_phase, False, ask)

    @pl.when(jnp.logical_not(has_left))
    def _():
        lax.fori_loop(0, own // ask, functools.partial(query_phase, True, ask), 0)
        lax.fori_loop(0, own, lone, 0)

    @pl.when(has_left)
    def _():
        early = me == 1
        lax.fori_loop(0, jnp.where(early, own, 0), passing, 0)
        lax.fori_loop(0, own // ask, batch, 0)

        @pl.when(early)
        def _():
            lax.fori_loop(0, own, ending, 0)

        @pl.when(jnp.logical_not(early))
        def _():
            lax.fori_loop(0, own, both, 0)

    for p in range(own):
        out_copy(p).wait_recv()
        out[peer_base + p] = out_recv[p] * gain_buf[...]
    for p in range(own):
        out_copy(p).wait_send()

    @pl.when(has_right)
    def _():
        for p in range(own):
            for h in range(PIECES):
                state_copy(p, h).wait_send()


def solution(mesh):
    n_seq, n_dim = mesh.shape["seq"], mesh.shape["dim"]
    hops = 1 if n_seq <= WINDOW + 1 else WINDOW

    def local(query, key, value, out_gate, beta, log_decay, lengths, norm_gain):
        seqs, heads, tokens, key_width = query.shape
        val_width = value.shape[2]
        val_total = val_width * n_dim
        pairs = seqs * heads
        own = pairs // n_dim
        half = tokens // 2
        group = max(g for g in range(1, GROUP + 1) if own % g == 0)
        lead = max(g for g in range(1, LEAD + 1) if group % g == 0)
        ask = max(g for g in range(1, ASK + 1) if own % g == 0)
        levels = (half // BASE).bit_length() - 1
        vmem = pl.BlockSpec(memory_space=pltpu.VMEM)
        anywhere = pl.BlockSpec(memory_space=pl.ANY)
        dma = pltpu.SemaphoreType.DMA
        flat = lambda x: x.reshape((pairs,) + x.shape[2:])
        hold = lambda x: pltpu.with_memory_space_constraint(x, pltpu.HBM)
        operands = [flat(value), flat(beta), flat(log_decay), norm_gain[None, :]]
        operands += [flat(query), flat(key), lengths.T]
        normed = pl.pallas_call(
            functools.partial(body, n_seq, hops, heads, val_total, group, lead, ask),
            out_shape=pltpu.VMEM((pairs, val_width, tokens), F32),
            in_specs=[anywhere] * 7,
            out_specs=vmem,
            scratch_shapes=[
                pltpu.SMEM((1, seqs), jnp.int32),
                pltpu.VMEM((pairs, val_width, tokens), BF16),
                pltpu.VMEM((pairs, tokens), F32),
                pltpu.VMEM((pairs, tokens), F32),
                pltpu.VMEM((1, val_width), F32),
                pltpu.VMEM((own, tokens, key_width), BF16),
                pltpu.VMEM((own, tokens, key_width), BF16),
                pltpu.VMEM((levels, half, tokens), BF16),
                pltpu.VMEM((tokens, tokens), BF16),
                pltpu.VMEM((3, half, half), F32),
                pltpu.VMEM((pairs, tokens), F32),
                pltpu.VMEM((pairs, tokens), F32),
                pltpu.VMEM((pairs, tokens), F32),
                pltpu.VMEM((val_width, tokens), F32),
                pltpu.VMEM((own, val_total + key_width, tokens), F32),
                pltpu.VMEM((own, key_width, key_width), BF16),
                pltpu.VMEM((own, key_width, key_width), BF16),
                pltpu.VMEM((own, val_total, tokens), F32),
                pltpu.VMEM((own, key_width, tokens), BF16),
                pltpu.VMEM((own, key_width, tokens), BF16),
                pltpu.VMEM((own, PIECES, hops, val_total // PIECES, key_width), F32),
                pltpu.VMEM((own, PIECES, hops, val_total // PIECES, key_width), F32),
                pltpu.VMEM((own, val_width, tokens), F32),
                pltpu.VMEM((own, val_width, tokens), F32),
                pltpu.VMEM((own, val_width, tokens), F32),
                pltpu.VMEM((own, val_width, tokens), F32),
                dma((7,)),
                dma((own // lead,)),
                dma((own, PIECES)),
                dma((own, PIECES)),
                dma((own,)),
                dma((own,)),
                dma((own,)),
                dma((own,)),
            ],
            compiler_params=pltpu.CompilerParams(
                collective_id=0, has_side_effects=True, vmem_limit_bytes=48 * 1024 * 1024
            ),
        )(*[hold(x) for x in operands])
        normed = normed.reshape(value.shape)
        gated = normed * jax.nn.silu(out_gate.astype(F32))
        return gated.astype(BF16)

    in_specs = (
        P("groups", "head", "seq", None),
        P("groups", "head", "seq", None),
        P("groups", "head", "dim", "seq"),
        P("groups", "head", "dim", "seq"),
        P("groups", "head", "seq"),
        P("groups", "head", "seq"),
        P("groups", "seq"),
        P("dim"),
    )
    out_specs = P("groups", "head", "dim", "seq")
    return jax.shard_map(local, mesh=mesh, in_specs=in_specs, out_specs=out_specs, check_vma=False)
```
